32 devices in a mesh: dp: 4 (over x, y), tp: 8 (over z, core).
Axes of the slice: x: 2, y: 2, z: 4, core: 2. Of those that a mesh axis runs over, the one named last changes fastest.
Arguments:
- x: bfloat16 [256, 2048], P('dp'), parts along dimension 0
- k_cache: bfloat16 [256, 2048, 16, 128], P('dp', None, 'tp'), parts along dimension 0
- v_cache: bfloat16 [256, 2048, 16, 128], P('dp', None, 'tp'), parts along dimension 0
- gain_a: bfloat16 [2048], replicated
- wq: bfloat16 [2048, 2048], P(None, 'tp')
- wo: bfloat16 [2048, 2048], P('tp')
- gain_m: bfloat16 [2048], replicated
- w_gate: bfloat16 [2048, 8192], P(None, 'tp')
- w_up: bfloat16 [2048, 8192], P(None, 'tp')
- w_down: bfloat16 [8192, 2048], P('tp')
Outputs:
- output: bfloat16 [256, 2048], P('dp'), parts along dimension 0
There are 4 independent parts. The reference program is written for one: setup_inputs(seed, part) draws one part's arguments, and reference() takes and returns one part's arrays. A program takes and returns all parts, laid end to end along the dimension named above; an argument that names none is the same for every part.
All inputs are finite; a program needn't handle non-finite values.
Results may differ from the reference program's by a relative error of at most 0.017.
Values are sent between devices in bfloat16 or wider.
A program may use at most 2 GiB of HBM per device.

```python
import jax
import jax.numpy as jnp
from jax import lax

BATCH = 64
CACHE = 2048
D = 2048
HEADS = 16
KV_HEADS = 16
HEAD = 128
FF = 8192
THETA = 10000


def setup_inputs(seed: int = 0, part: int = 0) -> dict:
    kx, kc, kw, kn, kq, ko, km, kg, ku, kd = jax.random.split(jax.random.key(seed), 10)
    kx, kc, kw = (jax.random.fold_in(k, part) for k in (kx, kc, kw))

    def weights(key, rows, columns):
        return jax.random.normal(key, (rows, columns), jnp.float32) * rows**-0.5

    drawn = {
        "x": jax.random.normal(kx, (BATCH, D), jnp.float32),
        "k_cache": 2 * jax.random.normal(kc, (BATCH, CACHE, KV_HEADS, HEAD), jnp.float32),
        "v_cache": 4 * jax.random.normal(kw, (BATCH, CACHE, KV_HEADS, HEAD), jnp.float32),
        "gain_a": 1 + 0.1 * jax.random.normal(kn, (D,), jnp.float32),
        "wq": 2 * weights(kq, D, HEADS * HEAD),
        "wo": weights(ko, HEADS * HEAD, D),
        "gain_m": 1 + 0.1 * jax.random.normal(km, (D,), jnp.float32),
        "w_gate": weights(kg, D, FF),
        "w_up": weights(ku, D, FF),
        "w_down": 2 * weights(kd, FF, D),
    }
    return {k: v.astype(jnp.bfloat16) for k, v in drawn.items()}


def normed(x, gain):
    wide = x.astype(jnp.float32)
    scale = lax.rsqrt(jnp.mean(wide * wide, -1, keepdims=True) + 1e-6)
    return (wide * scale * gain.astype(jnp.float32)).astype(jnp.bfloat16)


def turned(t, place, theta):
    half = t.shape[-1] // 2
    angle = place.astype(jnp.float32)[:, None] * theta ** (-jnp.arange(half, dtype=jnp.float32) / half)
    cos, sin = jnp.cos(angle)[:, None], jnp.sin(angle)[:, None]
    a, b = t[..., :half].astype(jnp.float32), t[..., half:].astype(jnp.float32)
    return jnp.concatenate([a * cos - b * sin, b * cos + a * sin], -1).astype(jnp.bfloat16)


def matmul(a, w):
    return jnp.dot(a, w, preferred_element_type=jnp.float32).astype(jnp.bfloat16)


def einsum(form, a, b):
    return jnp.einsum(form, a.astype(jnp.float32), b.astype(jnp.float32))


def seen_by(a, wq, k_cache, v_cache, head, theta):
    batch, cache, kv_heads = k_cache.shape[:3]
    place = jnp.full((batch,), cache - 1)
    q = turned(matmul(a, wq).reshape(batch, -1, head), place, theta).reshape(batch, kv_heads, -1, head)
    scores = einsum("bgsd,bugd->bgsu", q, k_cache) * head**-0.5
    weights = jax.nn.softmax(scores, -1).astype(jnp.bfloat16)
    return einsum("bgsu,bugd->bgsd", weights, v_cache).astype(jnp.bfloat16).reshape(batch, -1)


def hidden_of(b, w_gate, w_up):
    gate = jnp.dot(b, w_gate, preferred_element_type=jnp.float32)
    up = jnp.dot(b, w_up, preferred_element_type=jnp.float32)
    return (jax.nn.silu(gate) * up).astype(jnp.bfloat16)


def reference(x, k_cache, v_cache, gain_a, wq, wo, gain_m, w_gate, w_up, w_down):
    seen = seen_by(normed(x, gain_a), wq, k_cache, v_cache, HEAD, THETA)
    h = (x.astype(jnp.float32) + jnp.dot(seen, wo, preferred_element_type=jnp.float32)).astype(jnp.bfloat16)
    hidden = hidden_of(normed(h, gain_m), w_gate, w_up)
    return (h.astype(jnp.float32) + jnp.dot(hidden, w_down, preferred_element_type=jnp.float32)).astype(jnp.bfloat16)
```

```python
import jax
import jax.numpy as jnp
import numpy as np
from jax import lax
from jax.experimental import pallas as pl
from jax.experimental.pallas import tpu as pltpu
from jax.sharding import PartitionSpec as P

HEAD = 128
THETA = 10000
ROWS = 64
CACHE = 2048
D = 2048
HALF = D // 2
FF = 1024
KEYS = 2 * CACHE
PAIRS = ROWS // 2
SLOTS = 8
CHUNK = 16
STEP = CHUNK // 2
CHUNKS = ROWS // CHUNK
TILE = 256
TILES = KEYS // TILE
AT = (0, 1, 4, 5, 6, 9, 10)
F32, BF16 = jnp.float32, jnp.bfloat16


def dot(a, b):
    return jnp.dot(a, b, preferred_element_type=F32)


def wide_norm(wide, gain):
    scale = lax.rsqrt(jnp.mean(wide * wide, -1, keepdims=True) + 1e-6)
    return (wide * scale * gain).astype(BF16)


def one_hot(shape, hit):
    row, column = lax.broadcasted_iota(jnp.int32, shape, 0), lax.broadcasted_iota(jnp.int32, shape, 1)
    return jnp.where(hit(row, column), 1.0, 0.0).astype(BF16)


def kernel(x_in, k_in, v_in, ga_in, wq_in, wo_in, gm_in, wg_in, wu_in, wd_in, turn_in, y_out,
           x, kbuf, vbuf, ga, gm, turn, wq, wo, wg, wu, wd, queries, weights, results, hidden, term,
           sent, paired, summed, h, y, ksem, vsem, lsem, osem, pair_s, pair_r, z_s, z_r, done_s, done_r):
    me = lax.axis_index("tp")
    z, core = me // 2, me % 2
    partner = z * 2 + 1 - core

    def load_k(i, slot):
        return pltpu.make_async_copy(k_in.at[pl.ds(2 * i, 2)], kbuf.at[slot], ksem.at[slot])

    def load_v(i, slot):
        return pltpu.make_async_copy(v_in.at[pl.ds(2 * i, 2)], vbuf.at[slot], vsem.at[slot])

    first = [pltpu.make_async_copy(src, dst, lsem.at[n]) for n, (src, dst) in enumerate((
        (x_in.at[:, pl.ds(0, HALF)], x.at[0]), (x_in.at[:, pl.ds(HALF, HALF)], x.at[1]), (ga_in, ga), (turn_in, turn), (wq_in, wq)))]
    later = [pltpu.make_async_copy(src, dst, lsem.at[len(first) + n]) for n, (src, dst) in enumerate((
        (gm_in, gm), (wo_in, wo), (wg_in, wg), (wu_in, wu), (wd_in, wd)))]
    for copy in first:
        copy.start()
    for i in range(SLOTS):
        load_k(i, i).start()
        load_v(i, i).start()

    barrier = pltpu.get_barrier_semaphore()
    others = [lax.rem(z + n, 4) for n in (1, 2, 3)]
    for peer in [partner] + [2 * other + core for other in others]:
        pl.semaphore_signal(barrier, inc=1, device_id={"tp": peer}, device_id_type=pl.DeviceIdType.MESH)

    def gain_row(ref):
        wide = ref[...].astype(F32)
        return jnp.concatenate([wide[n:n + 1, :] for n in range(D // 128)], axis=1)

    for copy in first:
        copy.wait()
    a = wide_norm(jnp.concatenate([x[0], x[1]], axis=1).astype(F32), gain_row(ga))
    q = dot(a, wq[...]).astype(BF16).astype(F32)
    cos, sin = turn[0:1, :], turn[1:2, :]
    heads = [q[:, n * HEAD:(n + 1) * HEAD] for n in range(2)]
    stacked = jnp.concatenate([(t * cos + pltpu.roll(t, HEAD // 2, 1) * sin).astype(BF16) for t in heads], axis=0)
    left = one_hot((16 * PAIRS, 2 * ROWS), lambda r, c: (r % 16 == c // ROWS) & (c % ROWS == 2 * (r // 16)))
    right = one_hot((16 * PAIRS, 2 * ROWS), lambda r, c: (r % 16 == 2 + c // ROWS) & (c % ROWS == 2 * (r // 16) + 1))
    queries[:, 0:HEAD] = dot(left, stacked).astype(BF16)
    queries[:, HEAD:] = dot(right, stacked).astype(BF16)

    own = lax.broadcasted_iota(jnp.int32, (8, TILE), 0) % 2 == lax.broadcasted_iota(jnp.int32, (8, TILE), 1) % 2

    def scores(i, slot):
        pair = queries[pl.ds(pl.multiple_of(16 * i, 16), 16), :]
        out = []
        for t in range(TILES):
            at = pl.ds(t * TILE, TILE)
            keys = jnp.concatenate([kbuf[slot, 0, at, :], kbuf[slot, 1, at, :]], axis=1)
            s = lax.dot_general(pair, keys, (((1,), (1,)), ((), ())), preferred_element_type=F32)[0:8]
            out.append(jnp.where(own, s * HEAD**-0.5, -jnp.inf))
        return out

    def softmax(s):
        top = s[0]
        for t in s[1:]:
            top = jnp.maximum(top, t)
        top = jnp.max(top, -1, keepdims=True)
        e = [jnp.exp(t - top) for t in s]
        total = e[0]
        for t in e[1:]:
            total = total + t
        scale = 1.0 / jnp.sum(total, -1, keepdims=True)
        blank = jnp.zeros((8, TILE), F32)
        for t in range(TILES):
            weights[:, t * TILE:(t + 1) * TILE] = jnp.concatenate([e[t] * scale, blank], axis=0).astype(BF16)

    def values(i, slot):
        parts = [None, None]
        for t in range(TILES):
            at = pl.ds(t * TILE, TILE)
            v = jnp.concatenate([vbuf[slot, 0, at, :], vbuf[slot, 1, at, :]], axis=1)
            p = dot(weights[:, t * TILE:(t + 1) * TILE], v)
            parts[t % 2] = p if parts[t % 2] is None else parts[t % 2] + p
        results[pl.ds(pl.multiple_of(8 * i, 8), 8), :] = (parts[0] + parts[1])[0:8]

    load_k(0, 0).wait()
    softmax(scores(0, 0))
    load_k(SLOTS, 0).start()
    for copy in later:
        copy.start()

    pl.semaphore_wait(barrier, 4)

    def to_partner(src, dst, send, recv):
        return pltpu.make_async_remote_copy(src, dst, send, recv, device_id={"tp": partner}, device_id_type=pl.DeviceIdType.MESH)

    def to_chip(n, rnd, c, rows):
        return pltpu.make_async_remote_copy(
            summed.at[rnd, z, rows], summed.at[rnd, z, rows], z_s.at[rnd, c, n], z_r.at[rnd, c, z],
            device_id={"tp": 2 * others[n] + core}, device_id_type=pl.DeviceIdType.MESH)

    def from_chip(n, rnd, c, rows):
        other = others[n]
        return pltpu.make_async_remote_copy(
            summed.at[rnd, other, rows], summed.at[rnd, other, rows], z_s.at[rnd, c, n], z_r.at[rnd, c, other],
            device_id={"tp": 2 * other + core}, device_id_type=pl.DeviceIdType.MESH)

    def first_leg(rnd, c, rows):
        return to_partner(sent.at[rnd, rows], paired.at[rnd, rows], pair_s.at[rnd, c], pair_r.at[rnd, c])

    def send_term(rnd, c, rows):
        sent[rnd, rows, :] = term[rnd, 1 - core].astype(BF16)
        first_leg(rnd, c, rows).start()

    def second_leg(rnd, c, rows):
        first_leg(rnd, c, rows).wait()
        summed[rnd, z, rows, :] = (term[rnd, core] + paired[rnd, rows, :].astype(F32)).astype(BF16)
        for n in range(3):
            to_chip(n, rnd, c, rows).start()

    def third_leg(rnd, c, rows, base, out):
        for n in range(3):
            to_chip(n, rnd, c, rows).wait_send()
            from_chip(n, rnd, c, rows).wait_recv()
        total = summed[rnd, 0, rows, :].astype(F32)
        for n in range(1, 4):
            total = total + summed[rnd, n, rows, :].astype(F32)
        out[core, rows, :] = (base[core, rows, :].astype(F32) + total).astype(BF16)
        to_partner(out.at[core, rows], out.at[core, rows], done_s.at[rnd, c], done_r.at[rnd, c]).start()

    def finished(rnd, c, rows, out):
        to_partner(out.at[core, rows], out.at[core, rows], done_s.at[rnd, c], done_r.at[rnd, c]).wait_send()
        to_partner(out.at[1 - core, rows], out.at[1 - core, rows], done_s.at[rnd, c], done_r.at[rnd, c]).wait_recv()

    def project(c, rows):
        @pl.when(c == 0)
        def _():
            later[0].wait()
            later[1].wait()

        got = results[pl.ds(pl.multiple_of(8 * STEP * c, 8 * STEP), 8 * STEP), :].astype(BF16)
        seen = []
        for g in range(2):
            even = one_hot((CHUNK, 8 * STEP), lambda r, k: (r % 2 == 0) & (k == 8 * (r // 2) + g))
            odd = one_hot((CHUNK, 8 * STEP), lambda r, k: (r % 2 == 1) & (k == 8 * (r // 2) + 2 + g))
            seen.append((dot(even, got[:, 0:HEAD]) + dot(odd, got[:, HEAD:])).astype(BF16))
        seen = jnp.concatenate(seen, axis=1)
        for n in range(2):
            term[0, n] = dot(seen, wo[:, n * HALF:(n + 1) * HALF])
        send_term(0, c, rows)

    def mlp(c, rows):
        @pl.when(c == 0)
        def _():
            for copy in later[2:]:
                copy.wait()

        finished(0, c, rows, h)
        b = wide_norm(jnp.concatenate([h[0, rows, :], h[1, rows, :]], axis=1).astype(F32), gain_row(gm))

        @pl.loop(0, 2)
        def _(n):
            at = pl.ds(pl.multiple_of(n * (FF // 2), FF // 2), FF // 2)
            gate = dot(b, wg[:, at])
            hidden[:, at] = (gate * jax.nn.sigmoid(gate) * dot(b, wu[:, at])).astype(BF16)

        @pl.loop(0, 2)
        def _(n):
            term[1, n] = dot(hidden[...], wd[:, pl.ds(pl.multiple_of(n * HALF, HALF), HALF)])

        send_term(1, c, rows)

    def out_copy(n, c, rows):
        return pltpu.make_async_copy(y.at[n, rows], y_out.at[rows, pl.ds(n * HALF, HALF)], osem.at[n, c])

    def write(c, rows):
        finished(1, c, rows, y)
        for n in range(2):
            out_copy(n, c, rows).start()

    stages = (project, lambda c, rows: second_leg(0, c, rows), lambda c, rows: third_leg(0, c, rows, x, h), mlp,
              lambda c, rows: second_leg(1, c, rows), lambda c, rows: third_leg(1, c, rows, h, y), write)

    def iteration(i, _):
        @pl.when(i < PAIRS)
        def _():
            slot, before = i % SLOTS, (i - 1) % SLOTS
            load_k(i, slot).wait()
            load_v(i - 1, before).wait()
            s = scores(i, slot)
            values(i - 1, before)
            softmax(s)

            @pl.when(i + SLOTS < PAIRS)
            def _():
                load_k(i + SLOTS, slot).start()

            @pl.when(i - 1 + SLOTS < PAIRS)
            def _():
                load_v(i - 1 + SLOTS, before).start()

        @pl.when(i == PAIRS)
        def _():
            load_v(PAIRS - 1, (PAIRS - 1) % SLOTS).wait()
            values(PAIRS - 1, (PAIRS - 1) % SLOTS)

        for stage, at in zip(stages, AT):
            since = i - STEP - at

            @pl.when((since >= 0) & (since < STEP * CHUNKS) & (since % STEP == 0))
            def _():
                c = since // STEP
                stage(c, pl.ds(pl.multiple_of(c * CHUNK, CHUNK), CHUNK))

        return 0

    lax.fori_loop(1, PAIRS + AT[-1] + 1, iteration, 0)
    for c in range(CHUNKS):
        for n in range(2):
            out_copy(n, c, pl.ds(c * CHUNK, CHUNK)).wait()


def turn_table():
    angle = (CACHE - 1) * float(THETA) ** (-np.arange(HEAD // 2) / (HEAD // 2))
    cos, sin = np.cos(angle), np.sin(angle)
    table = np.zeros((8, HEAD), np.float32)
    table[0] = np.concatenate([cos, cos])
    table[1] = np.concatenate([-sin, sin])
    return table


def solution(mesh):
    def step(x, k_cache, v_cache, gain_a, wq, wo, gain_m, w_gate, w_up, w_down):
        dma, vmem = pltpu.SemaphoreType.DMA, pltpu.VMEM
        return pl.pallas_call(
            kernel,
            out_shape=jax.ShapeDtypeStruct((ROWS, D), BF16),
            in_specs=[pl.BlockSpec(memory_space=pl.ANY)] * 11,
            out_specs=pl.BlockSpec(memory_space=pl.ANY),
            scratch_shapes=[
                vmem((2, ROWS, HALF), BF16),
                vmem((SLOTS, 2, KEYS, HEAD), BF16), vmem((SLOTS, 2, KEYS, HEAD), BF16),
                vmem((D // 128, 128), BF16), vmem((D // 128, 128), BF16), vmem((8, HEAD), F32),
                vmem((D, 2 * HEAD), BF16), vmem((2 * HEAD, D), BF16), vmem((D, FF), BF16), vmem((D, FF), BF16), vmem((FF, D), BF16),
                vmem((16 * PAIRS, 2 * HEAD), BF16), vmem((16, KEYS), BF16), vmem((8 * PAIRS, 2 * HEAD), F32), vmem((CHUNK, FF), BF16),
                vmem((2, 2, CHUNK, HALF), F32),
                vmem((2, ROWS, HALF), BF16), vmem((2, ROWS, HALF), BF16), vmem((2, 4, ROWS, HALF), BF16),
                vmem((2, ROWS, HALF), BF16), vmem((2, ROWS, HALF), BF16),
                dma((SLOTS,)), dma((SLOTS,)), dma((10,)), dma((2, CHUNKS)),
                dma((2, CHUNKS)), dma((2, CHUNKS)), dma((2, CHUNKS, 3)), dma((2, CHUNKS, 4)), dma((2, CHUNKS)), dma((2, CHUNKS)),
            ],
            compiler_params=pltpu.CompilerParams(collective_id=0, has_side_effects=True, vmem_limit_bytes=60 * 2**20),
            name="layer",
        )(x, k_cache.reshape(ROWS, KEYS, HEAD), v_cache.reshape(ROWS, KEYS, HEAD), gain_a.reshape(D // 128, 128), wq, wo,
          gain_m.reshape(D // 128, 128), w_gate, w_up, w_down, jnp.asarray(turn_table()))

    states, cache, columns, rows_of = P("dp", None), P("dp", None, "tp", None), P(None, "tp"), P("tp", None)
    return jax.shard_map(
        step,
        mesh=mesh,
        in_specs=(states, cache, cache, P(None), columns, rows_of, P(None), columns, columns, rows_of),
        out_specs=states,
        check_vma=False,
    )
```

```python
import jax
import jax.numpy as jnp
import numpy as np
from jax import lax
from jax.experimental import pallas as pl
from jax.experimental.pallas import tpu as pltpu
from jax.sharding import PartitionSpec as P

HEAD = 128
THETA = 10000
ROWS = 64
CACHE = 2048
D = 2048
HALF = D // 2
FF = 1024
KEYS = 2 * CACHE
PAIRS = ROWS // 2
SLOTS = 8
CHUNK = 16
STEP = CHUNK // 2
CHUNKS = ROWS // CHUNK
TILE = 256
TILES = KEYS // TILE
AT = (0, 1, 7, 9, 10, 16, 17)
F32, BF16 = jnp.float32, jnp.bfloat16


def dot(a, b):
    return jnp.dot(a, b, preferred_element_type=F32)


def wide_norm(wide, gain):
    scale = lax.rsqrt(jnp.mean(wide * wide, -1, keepdims=True) + 1e-6)
    return (wide * scale * gain).astype(BF16)


def one_hot(shape, hit):
    row, column = lax.broadcasted_iota(jnp.int32, shape, 0), lax.broadcasted_iota(jnp.int32, shape, 1)
    return jnp.where(hit(row, column), 1.0, 0.0).astype(BF16)


def kernel(x_in, k_in, v_in, ga_in, wq_in, wo_in, gm_in, wg_in, wu_in, wd_in, turn_in, y_out,
           x, kbuf, vbuf, ga, gm, turn, wq, wo, wg, wu, wd, queries, logits, weights, results, term,
           sent, paired, summed, h, y, ksem, vsem, lsem, osem, pair_s, pair_r, z_s, z_r, done_s, done_r):
    me = lax.axis_index("tp")
    z, core = me // 2, me % 2
    partner = z * 2 + 1 - core

    def load_k(i, slot):
        return pltpu.make_async_copy(k_in.at[pl.ds(2 * i, 2)], kbuf.at[slot], ksem.at[slot])

    def load_v(i, slot):
        return pltpu.make_async_copy(v_in.at[pl.ds(2 * i, 2)], vbuf.at[slot], vsem.at[slot])

    first = [pltpu.make_async_copy(src, dst, lsem.at[n]) for n, (src, dst) in enumerate((
        (x_in.at[:, pl.ds(0, HALF)], x.at[0]), (x_in.at[:, pl.ds(HALF, HALF)], x.at[1]), (ga_in, ga), (turn_in, turn), (wq_in, wq)))]
    later = [pltpu.make_async_copy(src, dst, lsem.at[len(first) + n]) for n, (src, dst) in enumerate((
        (gm_in, gm), (wo_in, wo), (wg_in, wg), (wu_in, wu), (wd_in, wd)))]
    for copy in first:
        copy.start()
    for i in range(SLOTS):
        load_k(i, i).start()
        load_v(i, i).start()

    barrier = pltpu.get_barrier_semaphore()
    others = [lax.rem(z + n, 4) for n in (1, 2, 3)]
    for peer in [partner] + [2 * other + core for other in others]:
        pl.semaphore_signal(barrier, inc=1, device_id={"tp": peer}, device_id_type=pl.DeviceIdType.MESH)

    def gain_row(ref):
        wide = ref[...].astype(F32)
        return jnp.concatenate([wide[n:n + 1, :] for n in range(D // 128)], axis=1)

    for copy in first:
        copy.wait()
    a = wide_norm(jnp.concatenate([x[0], x[1]], axis=1).astype(F32), gain_row(ga))
    q = dot(a, wq[...]).astype(BF16).astype(F32)
    cos, sin = turn[0:1, :], turn[1:2, :]
    heads = [q[:, n * HEAD:(n + 1) * HEAD] for n in range(2)]
    stacked = jnp.concatenate([(t * cos + pltpu.roll(t, HEAD // 2, 1) * sin).astype(BF16) for t in heads], axis=0)
    left = one_hot((16 * PAIRS, 2 * ROWS), lambda r, c: (r % 16 == c // ROWS) & (c % ROWS == 2 * (r // 16)))
    right = one_hot((16 * PAIRS, 2 * ROWS), lambda r, c: (r % 16 == 2 + c // ROWS) & (c % ROWS == 2 * (r // 16) + 1))
    queries[:, 0:HEAD] = dot(left, stacked).astype(BF16)
    queries[:, HEAD:] = dot(right, stacked).astype(BF16)

    own = lax.broadcasted_iota(jnp.int32, (8, TILE), 0) % 2 == lax.broadcasted_iota(jnp.int32, (8, TILE), 1) % 2

    def scores(i, slot):
        pair = queries[pl.ds(pl.multiple_of(16 * i, 16), 16), :]
        for t in range(TILES):
            at = pl.ds(t * TILE, TILE)
            keys = jnp.concatenate([kbuf[slot, 0, at, :], kbuf[slot, 1, at, :]], axis=1)
            s = lax.dot_general(pair, keys, (((1,), (1,)), ((), ())), preferred_element_type=F32)[0:8]
            logits[:, t * TILE:(t + 1) * TILE] = jnp.where(own, s * HEAD**-0.5, -jnp.inf)

    def softmax():
        s = [logits[:, t * TILE:(t + 1) * TILE] for t in range(TILES)]
        top = s[0]
        for t in s[1:]:
            top = jnp.maximum(top, t)
        top = jnp.max(top, -1, keepdims=True)
        e = [jnp.exp(t - top) for t in s]
        total = e[0]
        for t in e[1:]:
            total = total + t
        scale = 1.0 / jnp.sum(total, -1, keepdims=True)
        blank = jnp.zeros((8, TILE), F32)
        return [jnp.concatenate([t * scale, blank], axis=0).astype(BF16) for t in e]

    def keep(w):
        for t in range(TILES):
            weights[:, t * TILE:(t + 1) * TILE] = w[t]

    def values(i, slot):
        parts = [None, None]
        for t in range(TILES):
            at = pl.ds(t * TILE, TILE)
            v = jnp.concatenate([vbuf[slot, 0, at, :], vbuf[slot, 1, at, :]], axis=1)
            p = dot(weights[:, t * TILE:(t + 1) * TILE], v)
            parts[t % 2] = p if parts[t % 2] is None else parts[t % 2] + p
        results[pl.ds(pl.multiple_of(8 * i, 8), 8), :] = (parts[0] + parts[1])[0:8]

    load_k(0, 0).wait()
    scores(0, 0)
    for copy in later:
        copy.start()
    load_k(SLOTS, 0).start()
    load_k(1, 1).wait()
    keep(softmax())
    scores(1, 1)
    load_k(SLOTS + 1, 1).start()

    pl.semaphore_wait(barrier, 4)

    def to_partner(src, dst, send, recv):
        return pltpu.make_async_remote_copy(src, dst, send, recv, device_id={"tp": partner}, device_id_type=pl.DeviceIdType.MESH)

    def to_chip(n, rnd, c, rows):
        return pltpu.make_async_remote_copy(
            summed.at[rnd, z, rows], summed.at[rnd, z, rows], z_s.at[rnd, c, n], z_r.at[rnd, c, z],
            device_id={"tp": 2 * others[n] + core}, device_id_type=pl.DeviceIdType.MESH)

    def from_chip(n, rnd, c, rows):
        other = others[n]
        return pltpu.make_async_remote_copy(
            summed.at[rnd, other, rows], summed.at[rnd, other, rows], z_s.at[rnd, c, n], z_r.at[rnd, c, other],
            device_id={"tp": 2 * other + core}, device_id_type=pl.DeviceIdType.MESH)

    def first_leg(rnd, c, rows):
        return to_partner(sent.at[rnd, rows], paired.at[rnd, rows], pair_s.at[rnd, c], pair_r.at[rnd, c])

    def send_term(rnd, c, rows, left, w):
        def half(n):
            return dot(left, w[:, pl.ds(pl.multiple_of(n * HALF, HALF), HALF)])

        sent[rnd, rows, :] = half(1 - core).astype(BF16)
        first_leg(rnd, c, rows).start()
        term[rnd] = half(core)

    def second_leg(rnd, c, rows):
        first_leg(rnd, c, rows).wait()
        summed[rnd, z, rows, :] = (term[rnd] + paired[rnd, rows, :].astype(F32)).astype(BF16)
        for n in range(3):
            to_chip(n, rnd, c, rows).start()

    def third_leg(rnd, c, rows, base, out):
        for n in range(3):
            to_chip(n, rnd, c, rows).wait_send()
            from_chip(n, rnd, c, rows).wait_recv()
        total = summed[rnd, 0, rows, :].astype(F32)
        for n in range(1, 4):
            total = total + summed[rnd, n, rows, :].astype(F32)
        out[core, rows, :] = (base[core, rows, :].astype(F32) + total).astype(BF16)
        to_partner(out.at[core, rows], out.at[core, rows], done_s.at[rnd, c], done_r.at[rnd, c]).start()

    def finished(rnd, c, rows, out):
        to_partner(out.at[core, rows], out.at[core, rows], done_s.at[rnd, c], done_r.at[rnd, c]).wait_send()
        to_partner(out.at[1 - core, rows], out.at[1 - core, rows], done_s.at[rnd, c], done_r.at[rnd, c]).wait_recv()

    def project(c, rows):
        @pl.when(c == 0)
        def _():
            later[0].wait()
            later[1].wait()

        got = results[pl.ds(pl.multiple_of(8 * STEP * c, 8 * STEP), 8 * STEP), :].astype(BF16)
        seen = []
        for g in range(2):
            even = one_hot((CHUNK, 8 * STEP), lambda r, k: (r % 2 == 0) & (k == 8 * (r // 2) + g))
            odd = one_hot((CHUNK, 8 * STEP), lambda r, k: (r % 2 == 1) & (k == 8 * (r // 2) + 2 + g))
            seen.append((dot(even, got[:, 0:HEAD]) + dot(odd, got[:, HEAD:])).astype(BF16))
        seen = jnp.concatenate(seen, axis=1)
        send_term(0, c, rows, seen, wo)

    def mlp(c, rows):
        @pl.when(c == 0)
        def _():
            for copy in later[2:]:
                copy.wait()

        finished(0, c, rows, h)
        b = wide_norm(jnp.concatenate([h[0, rows, :], h[1, rows, :]], axis=1).astype(F32), gain_row(gm))

        part = FF // 4
        hidden = []
        for n in range(4):
            gate = dot(b, wg[:, n * part:(n + 1) * part])
            hidden.append((gate * jax.nn.sigmoid(gate) * dot(b, wu[:, n * part:(n + 1) * part])).astype(BF16))
        send_term(1, c, rows, jnp.concatenate(hidden, axis=1), wd)

    def out_copy(n, c, rows):
        return pltpu.make_async_copy(y.at[n, rows], y_out.at[rows, pl.ds(n * HALF, HALF)], osem.at[n, c])

    def write(c, rows):
        finished(1, c, rows, y)
        for n in range(2):
            out_copy(n, c, rows).start()

    stages = (project, lambda c, rows: second_leg(0, c, rows), lambda c, rows: third_leg(0, c, rows, x, h), mlp,
              lambda c, rows: second_leg(1, c, rows), lambda c, rows: third_leg(1, c, rows, h, y), write)

    def iteration(i, _):
        @pl.when(i < PAIRS)
        def _():
            slot, before = i % SLOTS, (i - 2) % SLOTS
            load_k(i, slot).wait()
            load_v(i - 2, before).wait()
            values(i - 2, before)
            keep(softmax())
            scores(i, slot)

            @pl.when(i + SLOTS < PAIRS)
            def _():
                load_k(i + SLOTS, slot).start()

            @pl.when(i - 2 + SLOTS < PAIRS)
            def _():
                load_v(i - 2 + SLOTS, before).start()

        @pl.when(i == PAIRS)
        def _():
            load_v(PAIRS - 2, (PAIRS - 2) % SLOTS).wait()
            values(PAIRS - 2, (PAIRS - 2) % SLOTS)
            keep(softmax())

        @pl.when(i == PAIRS + 1)
        def _():
            load_v(PAIRS - 1, (PAIRS - 1) % SLOTS).wait()
            values(PAIRS - 1, (PAIRS - 1) % SLOTS)

        for stage, at in zip(stages, AT):
            since = i - STEP - 1 - at

            @pl.when((since >= 0) & (since < STEP * CHUNKS) & (since % STEP == 0))
            def _():
                c = since // STEP
                stage(c, pl.ds(pl.multiple_of(c * CHUNK, CHUNK), CHUNK))

        return 0

    lax.fori_loop(2, PAIRS + AT[-1] + 2, iteration, 0)
    for c in range(CHUNKS):
        for n in range(2):
            out_copy(n, c, pl.ds(c * CHUNK, CHUNK)).wait()


def turn_table():
    angle = (CACHE - 1) * float(THETA) ** (-np.arange(HEAD // 2) / (HEAD // 2))
    cos, sin = np.cos(angle), np.sin(angle)
    table = np.zeros((8, HEAD), np.float32)
    table[0] = np.concatenate([cos, cos])
    table[1] = np.concatenate([-sin, sin])
    return table


def solution(mesh):
    def step(x, k_cache, v_cache, gain_a, wq, wo, gain_m, w_gate, w_up, w_down):
        dma, vmem = pltpu.SemaphoreType.DMA, pltpu.VMEM
        return pl.pallas_call(
            kernel,
            out_shape=jax.ShapeDtypeStruct((ROWS, D), BF16),
            in_specs=[pl.BlockSpec(memory_space=pl.ANY)] * 11,
            out_specs=pl.BlockSpec(memory_space=pl.ANY),
            scratch_shapes=[
                vmem((2, ROWS, HALF), BF16),
                vmem((SLOTS, 2, KEYS, HEAD), BF16), vmem((SLOTS, 2, KEYS, HEAD), BF16),
                vmem((D // 128, 128), BF16), vmem((D // 128, 128), BF16), vmem((8, HEAD), F32),
                vmem((D, 2 * HEAD), BF16), vmem((2 * HEAD, D), BF16), vmem((D, FF), BF16), vmem((D, FF), BF16), vmem((FF, D), BF16),
                vmem((16 * PAIRS, 2 * HEAD), BF16), vmem((8, KEYS), F32), vmem((16, KEYS), BF16), vmem((8 * PAIRS, 2 * HEAD), F32),
                vmem((2, CHUNK, HALF), F32),
                vmem((2, ROWS, HALF), BF16), vmem((2, ROWS, HALF), BF16), vmem((2, 4, ROWS, HALF), BF16),
                vmem((2, ROWS, HALF), BF16), vmem((2, ROWS, HALF), BF16),
                dma((SLOTS,)), dma((SLOTS,)), dma((10,)), dma((2, CHUNKS)),
                dma((2, CHUNKS)), dma((2, CHUNKS)), dma((2, CHUNKS, 3)), dma((2, CHUNKS, 4)), dma((2, CHUNKS)), dma((2, CHUNKS)),
            ],
            compiler_params=pltpu.CompilerParams(collective_id=0, has_side_effects=True, vmem_limit_bytes=60 * 2**20),
            name="layer",
        )(x, k_cache.reshape(ROWS, KEYS, HEAD), v_cache.reshape(ROWS, KEYS, HEAD), gain_a.reshape(D // 128, 128), wq, wo,
          gain_m.reshape(D // 128, 128), w_gate, w_up, w_down, jnp.asarray(turn_table()))

    states, cache, columns, rows_of = P("dp", None), P("dp", None, "tp", None), P(None, "tp"), P("tp", None)
    return jax.shard_map(
        step,
        mesh=mesh,
        in_specs=(states, cache, cache, P(None), columns, rows_of, P(None), columns, columns, rows_of),
        out_specs=states,
        check_vma=False,
    )
```

```python
import jax
import jax.numpy as jnp
import numpy as np
from jax import lax
from jax.experimental import pallas as pl
from jax.experimental.pallas import tpu as pltpu
from jax.sharding import PartitionSpec as P

HEAD = 128
THETA = 10000
ROWS = 64
CACHE = 2048
D = 2048
HALF = D // 2
FF = 1024
KEYS = 2 * CACHE
PAIRS = ROWS // 2
SLOTS = 8
CHUNK = 8
UNROLL = 2
STEPS = PAIRS // UNROLL
STEP = CHUNK // 2 // UNROLL
CHUNKS = ROWS // CHUNK
TILE = 256
TILES = KEYS // TILE
TURNED = 8
AT = (0, 0, 3)
EARLY = (0, 5, 6)
GROUPS = ((0, 3, (12, 13, 19, 23)), (3, 2, (17, 18, 23, 24)), (5, 2, (18, 20, 24, 26)), (7, 1, (21, 22, 25, 26)))
F32, BF16 = jnp.float32, jnp.bfloat16
MESH = pl.DeviceIdType.MESH


def dot(a, b):
    return jnp.dot(a, b, preferred_element_type=F32)


def wide_norm(wide, gain):
    scale = lax.rsqrt(jnp.mean(wide * wide, -1, keepdims=True) + 1e-6)
    return (wide * scale * gain).astype(BF16)


def one_hot(shape, hit):
    row, column = lax.broadcasted_iota(jnp.int32, shape, 0), lax.broadcasted_iota(jnp.int32, shape, 1)
    return jnp.where(hit(row, column), 1.0, 0.0).astype(BF16)


def flat(t):
    return t.astype(F32).reshape(-1, t.shape[-1])


def whole(t):
    return jnp.concatenate([flat(t[0]), flat(t[1])], axis=1)


def kernel(x_in, k_in, v_in, ga_in, wq_in, wo_in, gm_in, wg_in, wu_in, wd_in, turn_in, y_out,
           x, kbuf, vbuf, ga, gm, turn, wq, wo, wg, wu, wd, queries, logits, weights, results, term, wide_term,
           sent, paired, summed, h, y, ksem, vsem, lsem, pair_s, pair_r, z_s, z_r, done_s, done_r):
    me = lax.axis_index("tp")
    z, core = me // 2, me % 2
    partner = z * 2 + 1 - core

    def load_k(i, slot):
        return pltpu.make_async_copy(k_in.at[pl.ds(2 * i, 2)], kbuf.at[slot], ksem.at[slot])

    def load_v(i, slot):
        return pltpu.make_async_copy(v_in.at[pl.ds(2 * i, 2)], vbuf.at[slot], vsem.at[slot])

    first = [pltpu.make_async_copy(src, dst, lsem.at[n]) for n, (src, dst) in enumerate((
        (x_in.at[:, :, pl.ds(0, HALF)], x.at[0]), (x_in.at[:, :, pl.ds(HALF, HALF)], x.at[1]), (ga_in, ga), (turn_in, turn), (wq_in, wq)))]
    later = [pltpu.make_async_copy(src, dst, lsem.at[len(first) + n]) for n, (src, dst) in enumerate((
        (gm_in, gm), (wo_in, wo), (wg_in, wg), (wu_in, wu), (wd_in, wd)))]
    for copy in first:
        copy.start()
    for i in range(SLOTS):
        load_k(i, i).start()
        load_v(i, i).start()

    barrier = pltpu.get_barrier_semaphore()
    others = [3 - z, lax.rem(z + 2, 4), z + 1 - 2 * (z % 2)]
    for peer in [partner] + [2 * other + core for other in others]:
        pl.semaphore_signal(barrier, inc=1, device_id={"tp": peer}, device_id_type=MESH)

    def gain_row(ref):
        wide = ref[...].astype(F32)
        return jnp.concatenate([wide[n:n + 1, :] for n in range(D // 128)], axis=1)

    for copy in first:
        copy.wait()
    a = wide_norm(whole(x[...]), gain_row(ga))
    q = dot(a, wq[...]).astype(BF16).astype(F32)
    cos, sin = turn[0:1, :], turn[1:2, :]
    heads = [q[:, n * HEAD:(n + 1) * HEAD] for n in range(2)]
    stacked = jnp.concatenate([(t * cos + pltpu.roll(t, HEAD // 2, 1) * sin).astype(BF16) for t in heads], axis=0)
    left = one_hot((16 * PAIRS, 2 * ROWS), lambda r, c: (r % 16 == c // ROWS) & (c % ROWS == 2 * (r // 16)))
    right = one_hot((16 * PAIRS, 2 * ROWS), lambda r, c: (r % 16 == 2 + c // ROWS) & (c % ROWS == 2 * (r // 16) + 1))
    queries[:, 0:HEAD] = dot(left, stacked).astype(BF16)
    queries[:, HEAD:] = dot(right, stacked).astype(BF16)

    own = lax.broadcasted_iota(jnp.int32, (8, TILE), 0) % 2 == lax.broadcasted_iota(jnp.int32, (8, TILE), 1) % 2

    def scores(i, slot, n):
        pair = queries[pl.ds(pl.multiple_of(16 * i, 16), 16), :]
        for t in range(TILES):
            at = pl.ds(t * TILE, TILE)
            halves = [kbuf[slot, half, at, :] for half in range(2)]
            if t * TURNED // TILES != (t + 1) * TURNED // TILES:
                s = dot(pair, jnp.concatenate([half.T for half in halves], axis=0))[0:8]
            else:
                keys = jnp.concatenate(halves, axis=1)
                s = lax.dot_general(pair, keys, (((1,), (1,)), ((), ())), preferred_element_type=F32)[0:8]
            logits[n, :, t * TILE:(t + 1) * TILE] = jnp.where(own, s * HEAD**-0.5, -jnp.inf)

    def softmax(n):
        s = [logits[n, :, t * TILE:(t + 1) * TILE] for t in range(TILES)]
        top = s[0]
        for t in s[1:]:
            top = jnp.maximum(top, t)
        top = jnp.max(top, -1, keepdims=True)
        e = [jnp.exp(t - top) for t in s]
        total = e[0]
        for t in e[1:]:
            total = total + t
        scale = 1.0 / jnp.sum(total, -1, keepdims=True)
        blank = jnp.zeros((8, TILE), F32)
        return [jnp.concatenate([t * scale, blank], axis=0).astype(BF16) for t in e]

    def keep(n, w):
        for t in range(TILES):
            weights[n, :, t * TILE:(t + 1) * TILE] = w[t]

    def values(i, slot, n):
        parts = [None, None]
        for t in range(TILES):
            at = pl.ds(t * TILE, TILE)
            v = jnp.concatenate([vbuf[slot, 0, at, :], vbuf[slot, 1, at, :]], axis=1)
            p = dot(weights[n, :, t * TILE:(t + 1) * TILE], v)
            parts[t % 2] = p if parts[t % 2] is None else parts[t % 2] + p
        results[i] = (parts[0] + parts[1])[0:8]

    two = range(UNROLL)
    for n in two:
        load_k(n, n).wait()
        scores(n, n, n)
    for copy in later:
        copy.start()
    for n in two:
        load_k(SLOTS + n, n).start()
    for n in two:
        load_k(UNROLL + n, UNROLL + n).wait()
    for n in two:
        keep(n, softmax(n))
        scores(UNROLL + n, UNROLL + n, n)
    for n in two:
        load_k(SLOTS + UNROLL + n, UNROLL + n).start()

    pl.semaphore_wait(barrier, 4)

    def to_partner(rnd, at, c):
        return pltpu.make_async_remote_copy(sent.at[rnd, at], paired.at[rnd, at], pair_s.at[rnd, c], pair_r.at[rnd, c],
                                            device_id={"tp": partner}, device_id_type=MESH)

    def to_chip(n, rnd, at, c):
        return pltpu.make_async_remote_copy(
            summed.at[rnd, z, at], summed.at[rnd, z, at], z_s.at[rnd, c, n], z_r.at[rnd, c, z],
            device_id={"tp": 2 * others[n] + core}, device_id_type=MESH)

    def from_chip(n, rnd, at, c):
        other = others[n]
        return pltpu.make_async_remote_copy(
            summed.at[rnd, other, at], summed.at[rnd, other, at], z_s.at[rnd, c, n], z_r.at[rnd, c, other],
            device_id={"tp": 2 * other + core}, device_id_type=MESH)

    def handed(rnd, half, at, c):
        out = (h, y)[rnd]
        return pltpu.make_async_remote_copy(out.at[half, at], out.at[half, at], done_s.at[rnd, c], done_r.at[rnd, c],
                                            device_id={"tp": partner}, device_id_type=MESH)

    def send_term(rnd, at, c, left, w, own):
        def half(n):
            return dot(left, w[:, pl.ds(pl.multiple_of(n * HALF, HALF), HALF)])

        sent[rnd, at] = half(1 - core).reshape(-1, CHUNK, HALF).astype(BF16)
        to_partner(rnd, at, c).start()
        own[...] = half(core)

    def over_pair(rnd, at, c, own):
        to_partner(rnd, at, c).wait()
        summed[rnd, z, at] = (own[...] + flat(paired[rnd, at])).reshape(-1, CHUNK, HALF).astype(BF16)
        for n in range(3):
            to_chip(n, rnd, at, c).start()

    def over_chips(rnd, at, c):
        for n in range(3):
            to_chip(n, rnd, at, c).wait_send()
            from_chip(n, rnd, at, c).wait_recv()
        total = summed[rnd, 0, at].astype(F32)
        for n in range(1, 4):
            total = total + summed[rnd, n, at].astype(F32)
        base, out = ((x, h), (h, y))[rnd]
        out[core, at] = (base[core, at].astype(F32) + total).astype(BF16)
        handed(rnd, core, at, c).start()

    def finished(rnd, at, c):
        handed(rnd, core, at, c).wait_send()
        handed(rnd, 1 - core, at, c).wait_recv()

    def project(c):
        @pl.when(c == 0)
        def _():
            later[0].wait()
            later[1].wait()

        got = [results[CHUNK // 2 * c + p] for p in range(CHUNK // 2)]
        heads = [jnp.concatenate([t[2 * n + g:2 * n + g + 1, n * HEAD:(n + 1) * HEAD] for t in got for n in range(2)], axis=0) for g in range(2)]
        seen = jnp.concatenate(heads, axis=1).astype(BF16)
        send_term(0, pl.ds(c, 1), c, seen, wo, term)

    chunk_stages = (project, lambda c: over_pair(0, pl.ds(c, 1), c, term), lambda c: over_chips(0, pl.ds(c, 1), c))

    def mlp(g, at, own):
        if g == 0:
            for copy in later[2:]:
                copy.wait()
        begin, size, _ = GROUPS[g]
        for c in range(begin, begin + size):
            finished(0, pl.ds(c, 1), c)
        b = wide_norm(whole(h[:, at]), gain_row(gm))
        part = FF // 4
        hidden = []
        for n in range(4):
            gate = dot(b, wg[:, n * part:(n + 1) * part])
            hidden.append((gate * jax.nn.sigmoid(gate) * dot(b, wu[:, n * part:(n + 1) * part])).astype(BF16))
        send_term(1, at, g, jnp.concatenate(hidden, axis=1), wd, own)

    def write(g, at):
        finished(1, at, g)
        for half in range(2):
            y_out[at, :, half * HALF:(half + 1) * HALF] = y[half, at]

    def iteration(i, _):
        @pl.when(i < STEPS)
        def _():
            keys, vals = [UNROLL * i + n for n in two], [UNROLL * (i - 2) + n for n in two]
            for k, v in zip(keys, vals):
                load_k(k, k % SLOTS).wait()
                load_v(v, v % SLOTS).wait()
            for n, v in enumerate(vals):
                values(v, v % SLOTS, n)
                keep(n, softmax(n))
            for n, k in enumerate(keys):
                scores(k, k % SLOTS, n)

            @pl.when(i + SLOTS // UNROLL < STEPS)
            def _():
                for k in keys:
                    load_k(k + SLOTS, k % SLOTS).start()

            @pl.when(i - 2 + SLOTS // UNROLL < STEPS)
            def _():
                for v in vals:
                    load_v(v + SLOTS, v % SLOTS).start()

        @pl.when(i == STEPS)
        def _():
            last = [UNROLL * (STEPS - 2) + n for n in two]
            for v in last:
                load_v(v, v % SLOTS).wait()
            for n, v in enumerate(last):
                values(v, v % SLOTS, n)
                keep(n, softmax(n))

        @pl.when(i == STEPS + 1)
        def _():
            @pl.loop(0, UNROLL)
            def _(n):
                v = UNROLL * (STEPS - 1) + n
                load_v(v, v % SLOTS).wait()
                values(v, v % SLOTS, n)

        for stage, after, early in zip(chunk_stages, AT, EARLY):
            since = i - STEP - 1 - after
            c = since // STEP

            @pl.when((since >= 0) & (c < CHUNKS) & (since - c * STEP == jnp.where(c < early, 1, 0)))
            def _():
                stage(c)

        @pl.when(i >= GROUPS[0][2][0])
        def _():
            for g, (begin, size, when) in enumerate(GROUPS):
                at, own = pl.ds(begin, size), wide_term.at[pl.ds(0, size * CHUNK)]
                group_stages = (lambda: mlp(g, at, own), lambda: over_pair(1, at, g, own), lambda: over_chips(1, at, g), lambda: write(g, at))
                for stage, now in zip(group_stages, when):
                    pl.when(i == now)(stage)

        return 0

    lax.fori_loop(2, GROUPS[-1][2][-1] + 1, iteration, 0)


def turn_table():
    angle = (CACHE - 1) * float(THETA) ** (-np.arange(HEAD // 2) / (HEAD // 2))
    cos, sin = np.cos(angle), np.sin(angle)
    table = np.zeros((8, HEAD), np.float32)
    table[0] = np.concatenate([cos, cos])
    table[1] = np.concatenate([-sin, sin])
    return table


def solution(mesh):
    def step(x, k_cache, v_cache, gain_a, wq, wo, gain_m, w_gate, w_up, w_down):
        dma, vmem = pltpu.SemaphoreType.DMA, pltpu.VMEM
        return pl.pallas_call(
            kernel,
            out_shape=jax.ShapeDtypeStruct((CHUNKS, CHUNK, D), BF16),
            in_specs=[pl.BlockSpec(memory_space=pl.ANY)] * 11,
            out_specs=pl.BlockSpec(memory_space=pltpu.VMEM),
            scratch_shapes=[
                vmem((2, CHUNKS, CHUNK, HALF), BF16),
                vmem((SLOTS, 2, KEYS, HEAD), BF16), vmem((SLOTS, 2, KEYS, HEAD), BF16),
                vmem((D // 128, 128), BF16), vmem((D // 128, 128), BF16), vmem((8, HEAD), F32),
                vmem((D, 2 * HEAD), BF16), vmem((2 * HEAD, D), BF16), vmem((D, FF), BF16), vmem((D, FF), BF16), vmem((FF, D), BF16),
                vmem((16 * PAIRS, 2 * HEAD), BF16), vmem((UNROLL, 8, KEYS), F32), vmem((UNROLL, 16, KEYS), BF16), vmem((PAIRS, 8, 2 * HEAD), F32),
                vmem((CHUNK, HALF), F32), vmem((GROUPS[0][1] * CHUNK, HALF), F32),
                vmem((2, CHUNKS, CHUNK, HALF), BF16), vmem((2, CHUNKS, CHUNK, HALF), BF16), vmem((2, 4, CHUNKS, CHUNK, HALF), BF16),
                vmem((2, CHUNKS, CHUNK, HALF), BF16), vmem((2, CHUNKS, CHUNK, HALF), BF16),
                dma((SLOTS,)), dma((SLOTS,)), dma((10,)),
                dma((2, CHUNKS)), dma((2, CHUNKS)), dma((2, CHUNKS, 3)), dma((2, CHUNKS, 4)), dma((2, CHUNKS)), dma((2, CHUNKS)),
            ],
            compiler_params=pltpu.CompilerParams(collective_id=0, has_side_effects=True, vmem_limit_bytes=52 * 2**20),
            name="layer",
        )(*[pltpu.with_memory_space_constraint(t, pltpu.HBM) for t in (
            x.reshape(CHUNKS, CHUNK, D), k_cache.reshape(ROWS, KEYS, HEAD), v_cache.reshape(ROWS, KEYS, HEAD), gain_a.reshape(D // 128, 128), wq, wo,
            gain_m.reshape(D // 128, 128), w_gate, w_up, w_down, jnp.asarray(turn_table()))]).reshape(ROWS, D)

    states, cache, columns, rows_of = P("dp", None), P("dp", None, "tp", None), P(None, "tp"), P("tp", None)
    return jax.shard_map(
        step,
        mesh=mesh,
        in_specs=(states, cache, cache, P(None), columns, rows_of, P(None), columns, columns, rows_of),
        out_specs=states,
        check_vma=False,
    )
```
